32 devices in a mesh: seq: 16 (over z, y, x), head: 2 (over core).
Axes of the slice: x: 2, y: 2, z: 4, core: 2. Of those that a mesh axis runs over, the one named last changes fastest.
Arguments:
- queries: bfloat16 [2048, 2048], P('seq', 'head'), may hold values from -6 to 6
- keys: bfloat16 [2048, 512], P('seq', 'head'), may hold values from -6 to 6
- values: bfloat16 [2048, 512], P('seq', 'head'), may hold values from -6 to 6
- tile_mask: int32 [32, 32], replicated, may hold values from 0 to 1, as said below
- out_weight: bfloat16 [2048, 4096], P('head'), may hold values from -0.5 to 0.5
Outputs:
- mixed: bfloat16 [2048, 4096], P(('seq', 'head'))
The draws below stay inside these ranges and needn't reach their ends.
Inputs may be any that keep to these rules, and one draw needn't show every extreme that they name: tile_mask[i, j] is 1 for i == j, 0 for j > i, and 0 or 1 below the diagonal.
All inputs are finite; a program needn't handle non-finite values.
Results may differ from the reference program's by a relative error of at most 0.01.
Values may be sent and summed in bfloat16 or wider, within the bound.
No kernel may reach another device: no remote copies, remote signals or barrier semaphores. Data moves between devices by JAX's collectives and lax.ppermute only.
A program may use at most 128 MiB of HBM per device.

```python
import math
import jax
import jax.numpy as jnp
from jax import lax

D = 4096
HD = 128
HEADS = 16
KVH = 4
TILE = 64
TOKENS = 2048
TILES = 32


def draw_field(key, salt, heads_count):
    base = jax.random.fold_in(key, salt)
    field = 1.5 * jax.random.truncated_normal(base, -4.0, 4.0, (TOKENS, heads_count * HD), jnp.float32)
    return field.astype(jnp.bfloat16)


def draw_queries(key, part):
    return draw_field(key, 1, HEADS)


def draw_keys(key, part):
    return draw_field(key, 2, KVH)


def draw_tile_mask(key, part):
    coin = jax.random.randint(jax.random.fold_in(key, 3), (TILES, TILES), 0, 2, dtype=jnp.int32)
    row_index = jnp.arange(TILES, dtype=jnp.int32)[:, None]
    column_index = jnp.arange(TILES, dtype=jnp.int32)[None, :]
    diagonal = jnp.where(row_index == column_index, 1, 0).astype(jnp.int32)
    return jnp.where(row_index > column_index, coin, diagonal).astype(jnp.int32)


def level_of(stream_key, dims, split, low, top_value):
    def one(axis_at, shards_of):
        heights = jax.random.uniform(jax.random.fold_in(jax.random.fold_in(stream_key, 6), axis_at), (shards_of,), jnp.float32, low / len(split), top_value / len(split))
        return jnp.repeat(jnp.exp(heights), dims[axis_at] // shards_of).reshape((-1,) + (1,) * (len(dims) - axis_at - 1))

    gain = one(*split[0])
    for cut in split[1:]:
        gain = gain * one(*cut)
    return gain


def scatter_about(stream_key, dims, deviation, reach, split=(), kind=jnp.bfloat16):
    result = deviation * jax.random.normal(stream_key, dims, jnp.float32)
    if split:
        result = result * level_of(stream_key, dims, split, -0.22, 0.18)
    return jnp.clip(result, -reach, reach).astype(kind)


def setup_inputs(seed: int = 0) -> dict:
    key_of = jax.random.split(jax.random.key(seed), 6)
    return {
        "queries": draw_queries(jax.random.fold_in(key_of[5], 71), 0),
        "keys": draw_keys(jax.random.fold_in(key_of[5], 71), 0),
        "values": scatter_about(key_of[2], (TOKENS, KVH * HD), 1.0, 6.0, ((0, 16), (1, 2))),
        "tile_mask": draw_tile_mask(jax.random.fold_in(key_of[5], 71), 0),
        "out_weight": scatter_about(key_of[4], (HEADS * HD, D), HD ** -0.5, 0.5, ((0, 2),)),
    }


MASK_FLOOR = -1e+30

def reference(queries, keys, values, tile_mask, out_weight):
    group = HEADS // KVH
    scale = 1.0 / math.sqrt(HD)
    query_field = queries.reshape(TOKENS, KVH, group, HD)
    key_field = keys.reshape(TOKENS, KVH, HD).astype(jnp.float32)
    value_field = values.reshape(TOKENS, KVH, HD).astype(jnp.float32)
    key_index = jnp.arange(TOKENS, dtype=jnp.int32)
    key_tile = key_index // TILE

    def one_tile(tile):
        row_start = (tile * TILE).astype(jnp.int32)
        query_tile = lax.dynamic_slice_in_dim(query_field, row_start, TILE, 0).astype(jnp.float32)
        query_index = row_start + jnp.arange(TILE, dtype=jnp.int32)
        mask_row = lax.dynamic_index_in_dim(tile_mask, tile, 0, keepdims=False)
        allowed = (mask_row[key_tile] > 0)[None, :] & (key_index[None, :] <= query_index[:, None])
        allowed_wide = allowed[:, None, None, :]
        scores = jnp.einsum('qgrd,kgd->qgrk', query_tile, key_field, precision=lax.Precision.HIGHEST) * scale
        masked = jnp.where(allowed_wide, scores, MASK_FLOOR)
        best = lax.optimization_barrier(jnp.max(masked, axis=-1, keepdims=True))
        weights = jnp.where(allowed_wide, jnp.exp(masked - best), 0.0)
        total = lax.optimization_barrier(jnp.sum(weights, axis=-1))
        rounded = lax.optimization_barrier(weights.astype(jnp.bfloat16)).astype(jnp.float32)
        blended = jnp.einsum('qgrk,kgd->qgrd', rounded, value_field, precision=lax.Precision.HIGHEST) / total[..., None]
        return blended.astype(jnp.bfloat16).reshape(TILE, HEADS * HD)
    attended = lax.map(one_tile, jnp.arange(TILES, dtype=jnp.int32)).reshape(TOKENS, HEADS * HD)
    return jnp.dot(attended, out_weight, preferred_element_type=jnp.float32).astype(jnp.bfloat16)
```

```python
import functools
import math

import jax
import jax.numpy as jnp
from jax import lax
from jax.experimental import pallas as pl
from jax.experimental.pallas import tpu as pltpu
from jax.sharding import PartitionSpec as P


HD = 128
TILE = 64
FLOOR = -1e30
GRANT = 60 * 1024 * 1024
STAGE = 2048
BOTH = ("seq", "head")
VMEM = pl.BlockSpec(memory_space=pltpu.VMEM)
HBM = pl.BlockSpec(memory_space=pl.ANY)


class Plan:
    def __init__(self, mesh, local_groups, group, rows, tiles):
        self.S, self.H = mesh.shape["seq"], mesh.shape["head"]
        self.L, self.group, self.rows, self.tiles = local_groups, group, rows, tiles
        self.g = self.L * self.H
        self.X = self.g // 2
        self.A = self.S // (2 * self.g)
        assert self.g % 2 == 0 and self.S % (2 * self.g) == 0

    def place(self, a, y, j):
        return ((a * 2 + j // self.X) * 2 + y) * self.X + j % self.X

    def split(self, s):
        x, y, b, a = s % self.X, s // self.X % 2, s // (2 * self.X) % 2, s // (4 * self.X)
        return a, y, b * self.X + x

    def flat(self, a, y, j, h):
        return self.place(a, y, j) * self.H + h

    def out_pairs(self, k, t):
        return [
            (self.flat(a, y, j, h), self.flat(a + k, y, h * self.L + (j % self.L + t) % self.L, j // self.L))
            for a in range(self.A - k)
            for y in range(2)
            for j in range(self.g)
            for h in range(self.H)
        ]

    def back_pairs(self, t):
        return [(b, a) for a, b in self.out_pairs(0, t)]

    def side_pairs(self):
        return [
            (self.flat(a, 1 - y, j, h), self.flat(a, y, j, h))
            for a in range(self.A)
            for y in range(2)
            for j in range(self.g)
            for h in range(self.H)
        ]

    def head_pairs(self, u):
        return [((c + u) % self.H, c) for c in range(self.H)]

    def far(self):
        return sorted(range(1, self.A), key=lambda k: -k * (self.A - k))

    def block(self, s, c, span, t):
        k, side, u = span
        a, y, i = self.split(s)
        j = (c + u) % self.H * self.L + (i + self.L - t) % self.L
        return self.place(a - k, y + side - 2 * y * side, j)


def dot_nt(a, b):
    return lax.dot_general(a, b, (((1,), (1,)), ((), ())), preferred_element_type=jnp.float32)


def tile_bias(plan, mask, s, c, spans, t):
    L, R, T = plan.L, plan.rows, plan.tiles
    first = plan.block(s, c, (0, 0, 0), t) * (R // TILE)
    pick = jnp.where(
        lax.broadcasted_iota(jnp.int32, (8, T), 1) == lax.broadcasted_iota(jnp.int32, (8, T), 0) + first, 1.0, 0.0
    ).astype(jnp.bfloat16)
    rows = jnp.dot(pick, mask, preferred_element_type=jnp.float32).astype(jnp.bfloat16)
    tile_of = lax.broadcasted_iota(jnp.int32, (T, R), 1) // TILE
    row_of = lax.broadcasted_iota(jnp.int32, (T, R), 0)
    part = []
    for span in spans:
        for tt in range(L):
            base = plan.block(s, c, span, tt) * (R // TILE)
            part.append(jnp.where(row_of == tile_of + base, 1.0, 0.0).astype(jnp.bfloat16))
    seen = jnp.dot(rows, jnp.concatenate(part, axis=1), preferred_element_type=jnp.float32)
    return jnp.where(seen > 0.5, 0.0, FLOOR)


def score_scale():
    return math.log2(math.e) / math.sqrt(HD)


def attend_body(plan, spans, where, count, whole, mask_ref, *refs):
    L, G, R = plan.L, plan.group, plan.rows
    n = len(spans)
    q_refs, refs = refs[:L], refs[L:]
    kv_refs, refs = refs[:count], refs[count:]
    out_refs, refs = refs[:L], refs[L:]
    if not whole:
        top_refs, refs = refs[:L], refs[L:]
    s_ref, b_ref, k_ref, v_ref = refs
    s, c = lax.axis_index("seq"), lax.axis_index("head")
    scale = score_scale()
    mask = mask_ref[...]
    W = L * R
    rts = R // TILE
    for t in range(L):
        b_ref[t] = tile_bias(plan, mask, s, c, spans, t)
    for m, span in enumerate(spans):
        for t in range(L):
            index, row = where[span, t]
            at = slice(m * W + t * R, m * W + (t + 1) * R)
            k_ref[at, :] = kv_refs[index][row : row + R, :HD]
            v_ref[at, :HD] = kv_refs[index][row : row + R, HD:]
    v_ref[:, HD:] = jnp.ones((n * W, HD), jnp.bfloat16)
    late = lax.broadcasted_iota(jnp.int32, (R, R), 1) > lax.broadcasted_iota(jnp.int32, (R, R), 0)
    corner = jnp.where(late, FLOOR, 0.0)
    for t in range(L):
        for e in range(G):
            q = q_refs[t][:, e * HD : (e + 1) * HD]
            high = None
            for m in range(n):
                sc = dot_nt(q, k_ref[m * W : (m + 1) * W, :])
                b = b_ref[t, :rts, m * W : (m + 1) * W]
                sc = (sc.reshape(rts, TILE, W) + b.reshape(rts, 1, W)).reshape(R, W)
                for tt in range(L):
                    x = sc[:, tt * R : (tt + 1) * R]
                    if spans[m] == (0, 0, 0) and tt == t:
                        x = x + corner
                    s_ref[:, m * W + tt * R : m * W + (tt + 1) * R] = x
                    high = x if high is None else jnp.maximum(high, x)
            top = jnp.max(high, axis=1, keepdims=True)
            total = None
            for m in range(n):
                w = jnp.exp2((s_ref[:, m * W : (m + 1) * W] - top) * scale).astype(jnp.bfloat16)
                d = jnp.dot(w, v_ref[m * W : (m + 1) * W, :], preferred_element_type=jnp.float32)
                total = d if total is None else total + d
            at = slice(e * HD, (e + 1) * HD)
            if whole:
                out_refs[t][:, at] = (total[:, :HD] / total[:, HD:]).astype(jnp.bfloat16)
            else:
                out_refs[t][e * R : (e + 1) * R, :] = total
                top_refs[t][e * R : (e + 1) * R, :] = jnp.broadcast_to(top, (R, HD))


def attend_stage(plan, spans, mask, q, kv, whole):
    L, G, R = plan.L, plan.group, plan.rows
    arrays, where = [], {}
    for span in spans:
        for t in range(L):
            array, row = kv[span, t]
            index = next((n for n, x in enumerate(arrays) if x is array), len(arrays))
            if index == len(arrays):
                arrays.append(array)
            where[span, t] = index, row
    keys = len(spans) * L * R
    if whole:
        shapes = [jax.ShapeDtypeStruct((R, G * HD), jnp.bfloat16)] * L
    else:
        shapes = [jax.ShapeDtypeStruct((G * R, 2 * HD), jnp.float32)] * L
        shapes += [jax.ShapeDtypeStruct((G * R, HD), jnp.float32)] * L
    return pl.pallas_call(
        functools.partial(attend_body, plan, spans, where, len(arrays), whole),
        out_shape=shapes,
        in_specs=[VMEM] * (1 + L + len(arrays)),
        out_specs=[VMEM] * len(shapes),
        scratch_shapes=[
            pltpu.VMEM((R, keys), jnp.float32),
            pltpu.VMEM((L, 8, keys), jnp.float32),
            pltpu.VMEM((keys, HD), jnp.bfloat16),
            pltpu.VMEM((keys, 2 * HD), jnp.bfloat16),
        ],
        compiler_params=pltpu.CompilerParams(vmem_limit_bytes=8 << 20),
        cost_estimate=pl.CostEstimate(flops=2 * L * G * R * keys * 3 * HD, bytes_accessed=0, transcendentals=0),
        name="attend",
    )(mask, *q, *arrays)


def attend(plan, spans, mask, q, kv):
    L, G, R = plan.L, plan.group, plan.rows
    step = max(1, STAGE // (L * R))
    if len(spans) <= step:
        return attend_stage(plan, spans, mask, q, kv, True)
    parts = [attend_stage(plan, spans[n : n + step], mask, q, kv, False) for n in range(0, len(spans), step)]
    outs = []
    for t in range(L):
        top = functools.reduce(jnp.maximum, [p[L + t][:, :1] for p in parts])
        total = sum(p[t] * jnp.exp2((p[L + t][:, :1] - top) * score_scale()) for p in parts)
        o = (total[:, :HD] / total[:, HD:]).astype(jnp.bfloat16)
        outs.append(o.reshape(G, R, HD).transpose(1, 0, 2).reshape(R, G * HD))
    return outs


def hold_body(w_ref, out_ref, sem):
    copy = pltpu.make_async_copy(w_ref, out_ref, sem)
    copy.start()
    copy.wait()


def hold(w):
    size = w.size * w.dtype.itemsize
    return pl.pallas_call(
        hold_body,
        out_shape=jax.ShapeDtypeStruct(w.shape, w.dtype),
        in_specs=[HBM],
        out_specs=VMEM,
        scratch_shapes=[pltpu.SemaphoreType.DMA],
        compiler_params=pltpu.CompilerParams(vmem_limit_bytes=GRANT - size * 17 // 8),
        cost_estimate=pl.CostEstimate(flops=1 << 20, bytes_accessed=0, transcendentals=0),
        name="hold",
    )(w)


def project_body(plan, cols, w_ref, *refs):
    L, H, R = plan.L, plan.H, plan.rows
    a_refs, (send_ref, own_ref, sum_ref) = refs[:L], refs[L:]
    h = lax.axis_index("head")
    _, _, j = plan.split(lax.axis_index("seq"))
    depth = a_refs[0].shape[1]
    part = R // H
    for n in range(own_ref.shape[1] // cols):
        at = slice(n * cols, (n + 1) * cols)
        total = None
        for t in range(L):
            w = w_ref[pl.ds(pl.multiple_of((j + t) % L * depth, depth), depth), at]
            d = jnp.dot(a_refs[t][...], w, preferred_element_type=jnp.float32)
            total = d if total is None else total + d
        sum_ref[:, at] = total
        own_ref[:, at] = sum_ref[pl.ds(pl.multiple_of(h * part, part), part), at]
        for u in range(1, H):
            to = (h + u) % H
            send_ref[(u - 1) * part : u * part, at] = sum_ref[pl.ds(pl.multiple_of(to * part, part), part), at].astype(
                jnp.bfloat16
            )


def project(plan, pieces, w):
    H, R = plan.H, plan.rows
    depth, D = w.shape
    part = R // H
    return pl.pallas_call(
        functools.partial(project_body, plan, 512),
        out_shape=[
            jax.ShapeDtypeStruct(((H - 1) * part, D), jnp.bfloat16),
            jax.ShapeDtypeStruct((part, D), jnp.float32),
        ],
        in_specs=[VMEM] * (1 + len(pieces)),
        out_specs=[VMEM] * 2,
        scratch_shapes=[pltpu.VMEM((R, D), jnp.float32)],
        compiler_params=pltpu.CompilerParams(vmem_limit_bytes=6 << 20),
        cost_estimate=pl.CostEstimate(flops=2 * R * depth * D, bytes_accessed=0, transcendentals=0),
        name="project",
    )(w, *pieces)


def layer(plan, queries, keys, values, tile_mask, out_weight):
    L, H, R = plan.L, plan.H, plan.rows
    wide = plan.group * HD
    _, _, j = plan.split(lax.axis_index("seq"))

    kv_send, q_send = [], []
    for t in range(L):
        p = (j + t) % L
        k_p = lax.dynamic_slice(keys, (0, p * HD), (R, HD))
        v_p = lax.dynamic_slice(values, (0, p * HD), (R, HD))
        kv_send.append(jnp.concatenate([k_p, v_p], axis=1))
        q_send.append(lax.dynamic_slice(queries, (0, p * wide), (R, wide)))
    mask = tile_mask.astype(jnp.bfloat16)
    weight = hold(out_weight)

    kv = {}
    side = plan.side_pairs()
    own = {(k, t): lax.ppermute(kv_send[t], BOTH, plan.out_pairs(k, t)) for k in [0, *plan.far()] for t in range(L)}
    near = jnp.concatenate([own[0, t] for t in range(L)], axis=0)
    near_side = lax.ppermute(near, BOTH, side)
    q = [lax.ppermute(q_send[t], BOTH, plan.out_pairs(0, t)) for t in range(L)]
    for t in range(L):
        kv[(0, 0, 0), t] = near, t * R
        kv[(0, 1, 0), t] = near_side, t * R
    both = jnp.concatenate([near, near_side], axis=0)
    for u in range(1, H):
        got = lax.ppermute(both, "head", plan.head_pairs(u))
        for t in range(L):
            kv[(0, 0, u), t] = got, t * R
            kv[(0, 1, u), t] = got, (L + t) * R
    for k in plan.far():
        far = [own[k, t] for t in range(L)]
        far_side = [lax.ppermute(far[t], BOTH, side) for t in range(L)]
        for t in range(L):
            kv[(k, 0, 0), t] = far[t], 0
            kv[(k, 1, 0), t] = far_side[t], 0
        for n, block in enumerate((far, far_side)):
            both = jnp.concatenate(block, axis=0)
            for u in range(1, H):
                got = lax.ppermute(both, "head", plan.head_pairs(u))
                for t in range(L):
                    kv[(k, n, u), t] = got, t * R
    spans = [(k, n, u) for k in [0, *plan.far()] for n in range(2) for u in range(H)]
    outs = attend(plan, spans, mask, q, kv)
    pieces = [lax.ppermute(outs[t], BOTH, plan.back_pairs(t)) for t in range(L)]
    send, mine = project(plan, pieces, weight)
    part = R // H
    for u in range(1, H):
        got = lax.ppermute(send[(u - 1) * part : u * part], "head", [(c, (c + u) % H) for c in range(H)])
        mine = mine + got.astype(jnp.float32)
    return mine.astype(jnp.bfloat16)


def solution(mesh):
    def program(queries, keys, values, tile_mask, out_weight):
        groups = keys.shape[1] // mesh.shape["head"] // HD
        rows = queries.shape[0] // mesh.shape["seq"]
        plan = Plan(mesh, groups, queries.shape[1] // keys.shape[1], rows, tile_mask.shape[0])

        def body(*args):
            return layer(plan, *args)

        step = jax.shard_map(
            body,
            mesh=mesh,
            in_specs=(P("seq", "head"), P("seq", "head"), P("seq", "head"), P(), P("head", None)),
            out_specs=P(("seq", "head"), None),
            check_vma=False,
        )
        return step(queries, keys, values, tile_mask, out_weight)

    return program
```

```python
import functools
import math

import jax
import jax.numpy as jnp
from jax import lax
from jax.experimental import pallas as pl
from jax.experimental.pallas import tpu as pltpu
from jax.sharding import PartitionSpec as P


HD = 128
TILE = 64
FLOOR = -1e30
GRANT = 60 * 1024 * 1024
STAGE = 2048
BOTH = ("seq", "head")
VMEM = pl.BlockSpec(memory_space=pltpu.VMEM)
HBM = pl.BlockSpec(memory_space=pl.ANY)


class Plan:
    def __init__(self, mesh, local_groups, group, rows, tiles):
        self.S, self.H = mesh.shape["seq"], mesh.shape["head"]
        self.L, self.group, self.rows, self.tiles = local_groups, group, rows, tiles
        self.g = self.L * self.H
        self.X = self.g // 2
        self.A = self.S // (2 * self.g)
        assert self.g % 2 == 0 and self.S % (2 * self.g) == 0

    def place(self, a, y, j):
        return ((a * 2 + j // self.X) * 2 + y) * self.X + j % self.X

    def split(self, s):
        x, y, b, a = s % self.X, s // self.X % 2, s // (2 * self.X) % 2, s // (4 * self.X)
        return a, y, b * self.X + x

    def flat(self, a, y, j, h):
        return self.place(a, y, j) * self.H + h

    def out_pairs(self, k, t):
        return [
            (self.flat(a, y, j, h), self.flat(a + k, y, h * self.L + (j % self.L + t) % self.L, j // self.L))
            for a in range(self.A - k)
            for y in range(2)
            for j in range(self.g)
            for h in range(self.H)
        ]

    def back_pairs(self, t):
        return [(b, a) for a, b in self.out_pairs(0, t)]

    def side_pairs(self):
        return [
            (self.flat(a, 1 - y, j, h), self.flat(a, y, j, h))
            for a in range(self.A)
            for y in range(2)
            for j in range(self.g)
            for h in range(self.H)
        ]

    def head_pairs(self, u):
        return [((c + u) % self.H, c) for c in range(self.H)]

    def far(self):
        return sorted(range(1, self.A), key=lambda k: -k * (self.A - k))

    def block(self, s, c, span, t):
        k, side, u = span
        a, y, i = self.split(s)
        j = (c + u) % self.H * self.L + (i + self.L - t) % self.L
        return self.place(a - k, y + side - 2 * y * side, j)


def dot_nt(a, b):
    return lax.dot_general(a, b, (((1,), (1,)), ((), ())), preferred_element_type=jnp.float32)


def tile_bias(plan, mask, s, c, spans, t):
    L, R, T = plan.L, plan.rows, plan.tiles
    first = plan.block(s, c, (0, 0, 0), t) * (R // TILE)
    pick = jnp.where(
        lax.broadcasted_iota(jnp.int32, (8, T), 1) == lax.broadcasted_iota(jnp.int32, (8, T), 0) + first, 1.0, 0.0
    ).astype(jnp.bfloat16)
    rows = jnp.dot(pick, mask, preferred_element_type=jnp.float32).astype(jnp.bfloat16)
    tile_of = lax.broadcasted_iota(jnp.int32, (T, R), 1) // TILE
    row_of = lax.broadcasted_iota(jnp.int32, (T, R), 0)
    part = []
    for span in spans:
        for tt in range(L):
            base = plan.block(s, c, span, tt) * (R // TILE)
            part.append(jnp.where(row_of == tile_of + base, 1.0, 0.0).astype(jnp.bfloat16))
    seen = jnp.dot(rows, jnp.concatenate(part, axis=1), preferred_element_type=jnp.float32)
    return jnp.where(seen > 0.5, 0.0, FLOOR)


def score_scale():
    return math.log2(math.e) / math.sqrt(HD)


def fill_keys(plan, spans, where, kv_refs, k_ref, v_ref):
    L, R = plan.L, plan.rows
    for m, span in enumerate(spans):
        for t in range(L):
            index, row = where[span, t]
            at = slice((m * L + t) * R, (m * L + t + 1) * R)
            k_ref[at, :] = kv_refs[index][row : row + R, :HD]
            v_ref[at, :HD] = kv_refs[index][row : row + R, HD:]
    v_ref[:, HD:] = jnp.ones((v_ref.shape[0], HD), jnp.bfloat16)


def attend_piece(plan, spans, t, s, c, mask, q_ref, k_ref, v_ref, s_ref, b_ref, write):
    L, G, R = plan.L, plan.group, plan.rows
    n, W, rts = len(spans), L * R, R // TILE
    scale = score_scale()
    b_ref[...] = tile_bias(plan, mask, s, c, spans, t)
    late = lax.broadcasted_iota(jnp.int32, (R, R), 1) > lax.broadcasted_iota(jnp.int32, (R, R), 0)
    corner = jnp.where(late, FLOOR, 0.0)
    for e in range(G):
        q = q_ref[:, (2 + e) * HD : (3 + e) * HD]
        high = None
        for m in range(n):
            sc = dot_nt(q, k_ref[m * W : (m + 1) * W, :])
            b = b_ref[:rts, m * W : (m + 1) * W]
            sc = (sc.reshape(rts, TILE, W) + b.reshape(rts, 1, W)).reshape(R, W)
            for tt in range(L):
                x = sc[:, tt * R : (tt + 1) * R]
                if spans[m] == (0, 0, 0) and tt == t:
                    x = x + corner
                s_ref[:, m * W + tt * R : m * W + (tt + 1) * R] = x
                high = x if high is None else jnp.maximum(high, x)
        top = jnp.max(high, axis=1, keepdims=True)
        total = None
        for m in range(n):
            w = jnp.exp2((s_ref[:, m * W : (m + 1) * W] - top) * scale).astype(jnp.bfloat16)
            d = jnp.dot(w, v_ref[m * W : (m + 1) * W, :], preferred_element_type=jnp.float32)
            total = d if total is None else total + d
        write(e, total, top)


def index_of(plan, spans, kv):
    arrays, where = [], {}
    for span in spans:
        for t in range(plan.L):
            array, row = kv[span, t]
            index = next((n for n, x in enumerate(arrays) if x is array), len(arrays))
            if index == len(arrays):
                arrays.append(array)
            where[span, t] = index, row
    return arrays, where


def stage_body(plan, spans, where, count, mask_ref, *refs):
    L, R = plan.L, plan.rows
    q_refs, refs = refs[:L], refs[L:]
    kv_refs, refs = refs[:count], refs[count:]
    out_refs, top_refs, (s_ref, b_ref, k_ref, v_ref) = refs[:L], refs[L : 2 * L], refs[2 * L :]
    s, c = lax.axis_index("seq"), lax.axis_index("head")
    fill_keys(plan, spans, where, kv_refs, k_ref, v_ref)
    for t in range(L):

        def write(e, total, top, t=t):
            out_refs[t][e * R : (e + 1) * R, :] = total
            top_refs[t][e * R : (e + 1) * R, :] = jnp.broadcast_to(top, (R, HD))

        attend_piece(plan, spans, t, s, c, mask_ref[...], q_refs[t], k_ref, v_ref, s_ref, b_ref, write)


def attend_stage(plan, spans, mask, q, kv):
    L, G, R = plan.L, plan.group, plan.rows
    arrays, where = index_of(plan, spans, kv)
    keys = len(spans) * L * R
    shapes = [jax.ShapeDtypeStruct((G * R, 2 * HD), jnp.float32)] * L
    shapes += [jax.ShapeDtypeStruct((G * R, HD), jnp.float32)] * L
    return pl.pallas_call(
        functools.partial(stage_body, plan, spans, where, len(arrays)),
        out_shape=shapes,
        in_specs=[VMEM] * (1 + L + len(arrays)),
        out_specs=[VMEM] * len(shapes),
        scratch_shapes=[
            pltpu.VMEM((R, keys), jnp.float32),
            pltpu.VMEM((8, keys), jnp.float32),
            pltpu.VMEM((keys, HD), jnp.bfloat16),
            pltpu.VMEM((keys, 2 * HD), jnp.bfloat16),
        ],
        compiler_params=pltpu.CompilerParams(vmem_limit_bytes=12 << 20),
        name="stage",
    )(mask, *q, *arrays)


def piece_body(plan, spans, t, where, count, mask_ref, q_ref, *refs):
    kv_refs, refs = refs[:count], refs[count:]
    if where is None:
        k_ref, v_ref = kv_refs
        out_ref, s_ref, b_ref = refs
    else:
        out_ref, k_ref, v_ref, s_ref, b_ref = refs
    s, c = lax.axis_index("seq"), lax.axis_index("head")
    if where is not None:
        fill_keys(plan, spans, where, kv_refs, k_ref, v_ref)

    def write(e, total, top):
        out_ref[:, e * HD : (e + 1) * HD] = (total[:, :HD] / total[:, HD:]).astype(jnp.bfloat16)

    attend_piece(plan, spans, t, s, c, mask_ref[...], q_ref, k_ref, v_ref, s_ref, b_ref, write)


def attend_one(plan, spans, t, mask, q, kv, where):
    L, G, R = plan.L, plan.group, plan.rows
    keys = len(spans) * L * R
    shapes = [jax.ShapeDtypeStruct((R, G * HD), jnp.bfloat16)]
    if where is not None:
        shapes += [jax.ShapeDtypeStruct((keys, HD), jnp.bfloat16), jax.ShapeDtypeStruct((keys, 2 * HD), jnp.bfloat16)]
    return pl.pallas_call(
        functools.partial(piece_body, plan, spans, t, where, len(kv)),
        out_shape=shapes,
        in_specs=[VMEM] * (2 + len(kv)),
        out_specs=[VMEM] * len(shapes),
        scratch_shapes=[pltpu.VMEM((R, keys), jnp.float32), pltpu.VMEM((8, keys), jnp.float32)],
        compiler_params=pltpu.CompilerParams(vmem_limit_bytes=6 << 20),
        cost_estimate=pl.CostEstimate(flops=2 * G * R * keys * 3 * HD, bytes_accessed=0, transcendentals=0),
    )(mask, q, *kv)


def attend_staged(plan, spans, mask, q, kv):
    L, G, R = plan.L, plan.group, plan.rows
    step = max(1, STAGE // (L * R))
    parts = [attend_stage(plan, spans[n : n + step], mask, q, kv) for n in range(0, len(spans), step)]
    outs = []
    for t in range(L):
        top = functools.reduce(jnp.maximum, [p[L + t][:, :1] for p in parts])
        total = sum(p[t] * jnp.exp2((p[L + t][:, :1] - top) * score_scale()) for p in parts)
        o = (total[:, :HD] / total[:, HD:]).astype(jnp.bfloat16)
        outs.append(o.reshape(G, R, HD).transpose(1, 0, 2).reshape(R, G * HD))
    return outs


def hold_body(plan, t, w_ref, *refs):
    _, _, j = plan.split(lax.axis_index("seq"))
    if t == 0:
        mask_ref, out_ref, open_ref, raw_ref, sem = refs
    else:
        out_ref, sem = refs
    depth = out_ref.shape[0]
    here = pl.ds(pl.multiple_of((j + t) % plan.L * depth, depth), depth)
    copies = [pltpu.make_async_copy(w_ref.at[here, :], out_ref, sem.at[0])]
    if t == 0:
        copies.append(pltpu.make_async_copy(mask_ref, raw_ref, sem.at[1]))
    for copy in copies:
        copy.start()
    for copy in copies:
        copy.wait()
    if t == 0:
        open_ref[...] = raw_ref[...].astype(jnp.float32).astype(jnp.bfloat16)


def hold(plan, t, w, *mask):
    depth, D = w.shape[0] // plan.L, w.shape[1]
    size = w.size * w.dtype.itemsize
    shapes = [jax.ShapeDtypeStruct((depth, D), w.dtype)] + [jax.ShapeDtypeStruct(m.shape, jnp.bfloat16) for m in mask]
    return pl.pallas_call(
        functools.partial(hold_body, plan, t),
        out_shape=shapes,
        in_specs=[HBM] * (1 + len(mask)),
        out_specs=[VMEM] * len(shapes),
        scratch_shapes=[pltpu.VMEM(m.shape, m.dtype) for m in mask] + [pltpu.SemaphoreType.DMA((2,))],
        compiler_params=pltpu.CompilerParams(vmem_limit_bytes=GRANT - size * (6 + t) // 4),
        cost_estimate=pl.CostEstimate(flops=1 << 20, bytes_accessed=0, transcendentals=0),
    )(w, *mask)


def project_body(plan, cols, w_ref, a_ref, *refs):
    H, R = plan.H, plan.rows
    h = lax.axis_index("head")
    part = R // H
    for n in range(w_ref.shape[1] // cols):
        at = slice(n * cols, (n + 1) * cols)
        d = jnp.dot(a_ref[...], w_ref[:, at], preferred_element_type=jnp.float32)
        if len(refs) == 1:
            refs[0][:, at] = d
            continue
        sum_ref, send_ref, own_ref, all_ref = refs
        all_ref[:, at] = sum_ref[:, at] + d
        own_ref[:, at] = all_ref[pl.ds(pl.multiple_of(h * part, part), part), at]
        for u in range(1, H):
            to = (h + u) % H
            send_ref[(u - 1) * part : u * part, at] = all_ref[pl.ds(pl.multiple_of(to * part, part), part), at].astype(
                jnp.bfloat16
            )


def project(plan, t, piece, w, total):
    H, R = plan.H, plan.rows
    depth, D = piece.shape[1], w.shape[1]
    part = R // H
    last = t == plan.L - 1
    if last:
        shapes = [
            jax.ShapeDtypeStruct(((H - 1) * part, D), jnp.bfloat16),
            jax.ShapeDtypeStruct((part, D), jnp.float32),
        ]
    else:
        shapes = [jax.ShapeDtypeStruct((R, D), jnp.float32)]
    args = [w, piece] + ([total] if last else [])
    return pl.pallas_call(
        functools.partial(project_body, plan, 512),
        out_shape=shapes,
        in_specs=[VMEM] * len(args),
        out_specs=[VMEM] * len(shapes),
        scratch_shapes=[pltpu.VMEM((R, D), jnp.float32)] if last else [],
        compiler_params=pltpu.CompilerParams(vmem_limit_bytes=6 << 20),
        cost_estimate=pl.CostEstimate(flops=2 * R * depth * D, bytes_accessed=0, transcendentals=0),
        name="project",
    )(*args)


def layer(plan, queries, keys, values, tile_mask, out_weight):
    L, H, R = plan.L, plan.H, plan.rows
    wide = plan.group * HD
    _, _, j = plan.split(lax.axis_index("seq"))

    kv_send, full_send = [], []
    for t in range(L):
        p = (j + t) % L
        k_p = lax.dynamic_slice(keys, (0, p * HD), (R, HD))
        v_p = lax.dynamic_slice(values, (0, p * HD), (R, HD))
        q_p = lax.dynamic_slice(queries, (0, p * wide), (R, wide))
        kv_send.append(jnp.concatenate([k_p, v_p], axis=1))
        full_send.append(jnp.concatenate([k_p, v_p, q_p], axis=1))
    first_weight, mask = hold(plan, 0, out_weight, tile_mask)
    weights = [first_weight]
    for t in range(1, L):
        weights += hold(plan, t, out_weight)

    kv = {}
    side = plan.side_pairs()
    own = {}
    for k in [0, *plan.far()]:
        for t in range(L):
            own[k, t] = lax.ppermute(kv_send[t] if k else full_send[t], BOTH, plan.out_pairs(k, t))
    q = [own[0, t] for t in range(L)]
    near = jnp.concatenate([own[0, t][:, : 2 * HD] for t in range(L)], axis=0)
    near_side = lax.ppermute(near, BOTH, side)
    for t in range(L):
        kv[(0, 0, 0), t] = near, t * R
        kv[(0, 1, 0), t] = near_side, t * R
    both = jnp.concatenate([near, near_side], axis=0)
    for u in range(1, H):
        got = lax.ppermute(both, "head", plan.head_pairs(u))
        for t in range(L):
            kv[(0, 0, u), t] = got, t * R
            kv[(0, 1, u), t] = got, (L + t) * R
    for k in plan.far():
        far = jnp.concatenate([own[k, t] for t in range(L)], axis=0)
        far_side = lax.ppermute(far, BOTH, side)
        for n, block in enumerate((far, far_side)):
            got = {u: lax.ppermute(block, "head", plan.head_pairs(u)) for u in range(1, H)}
            for u in range(H):
                for t in range(L):
                    kv[(k, n, u), t] = got[u] if u else block, t * R
    spans = [(k, n, u) for k in [0, *plan.far()] for n in range(2) for u in range(H)]
    pieces = []
    if len(spans) * L * R <= STAGE:
        laid, where = index_of(plan, spans, kv)
        for t in range(L):
            out, *more = attend_one(plan, spans, t, mask, q[t], laid, where)
            if where is not None:
                laid, where = more, None
            pieces.append(lax.ppermute(out, BOTH, plan.back_pairs(t)))
    else:
        outs = attend_staged(plan, spans, mask, q, kv)
        for t in range(L):
            pieces.append(lax.ppermute(outs[t], BOTH, plan.back_pairs(t)))
    total = None
    for t in range(L):
        res = project(plan, t, pieces[t], weights[t], total)
        total = res[0]
    send, mine = res
    part = R // H
    for u in range(1, H):
        got = lax.ppermute(send[(u - 1) * part : u * part], "head", [(c, (c + u) % H) for c in range(H)])
        mine = mine + got.astype(jnp.float32)
    return mine.astype(jnp.bfloat16)


def solution(mesh):
    def program(queries, keys, values, tile_mask, out_weight):
        groups = keys.shape[1] // mesh.shape["head"] // HD
        rows = queries.shape[0] // mesh.shape["seq"]
        plan = Plan(mesh, groups, queries.shape[1] // keys.shape[1], rows, tile_mask.shape[0])

        def body(*args):
            return layer(plan, *args)

        step = jax.shard_map(
            body,
            mesh=mesh,
            in_specs=(P("seq", "head"), P("seq", "head"), P("seq", "head"), P(), P("head", None)),
            out_specs=P(("seq", "head"), None),
            check_vma=False,
        )
        return step(queries, keys, values, tile_mask, out_weight)

    return program
```

```python
import functools
import math

import jax
import jax.numpy as jnp
from jax import lax
from jax.experimental import pallas as pl
from jax.experimental.pallas import tpu as pltpu
from jax.sharding import PartitionSpec as P


HD = 128
TILE = 64
FLOOR = -1e30
GRANT = 60 * 1024 * 1024
STAGE = 2048
BOTH = ("seq", "head")
VMEM = pl.BlockSpec(memory_space=pltpu.VMEM)
HBM = pl.BlockSpec(memory_space=pl.ANY)


class Plan:
    def __init__(self, mesh, local_groups, group, rows, tiles):
        self.S, self.H = mesh.shape["seq"], mesh.shape["head"]
        self.L, self.group, self.rows, self.tiles = local_groups, group, rows, tiles
        self.g = self.L * self.H
        self.A = self.S // (2 * self.g)
        assert self.S % (2 * self.g) == 0

    def place(self, a, y, j):
        return (a * 2 + y) * self.g + j

    def split(self, s):
        return s // (2 * self.g), s // self.g % 2, s % self.g

    def flat(self, a, y, j, h):
        return self.place(a, y, j) * self.H + h

    def out_pairs(self, k, t):
        return [
            (self.flat(a, y, j, h), self.flat(a + k, y, h * self.L + (j % self.L + t) % self.L, (j // self.L + 1) % self.H))
            for a in range(self.A - k)
            for y in range(2)
            for j in range(self.g)
            for h in range(self.H)
        ]

    def back_pairs(self, t):
        return [(b, a) for a, b in self.out_pairs(0, t)]

    def side_pairs(self):
        return [
            (self.flat(a, 1 - y, j, h), self.flat(a, y, j, h))
            for a in range(self.A)
            for y in range(2)
            for j in range(self.g)
            for h in range(self.H)
        ]

    def head_pairs(self, u):
        return [((c + u) % self.H, c) for c in range(self.H)]

    def far(self):
        return sorted(range(1, self.A), key=lambda k: -k * (self.A - k))

    def block(self, s, c, span, t):
        k, side, u = span
        a, y, i = self.split(s)
        j = (c + u + self.H - 1) % self.H * self.L + (i + self.L - t) % self.L
        return self.place(a - k, y + side - 2 * y * side, j)


def dot_nt(a, b):
    return lax.dot_general(a, b, (((1,), (1,)), ((), ())), preferred_element_type=jnp.float32)


def tile_bias(plan, mask, s, c, spans, t):
    L, R, T = plan.L, plan.rows, plan.tiles
    first = plan.block(s, c, (0, 0, 0), t) * (R // TILE)
    pick = jnp.where(
        lax.broadcasted_iota(jnp.int32, (8, T), 1) == lax.broadcasted_iota(jnp.int32, (8, T), 0) + first, 1.0, 0.0
    ).astype(jnp.bfloat16)
    rows = jnp.dot(pick, mask, preferred_element_type=jnp.float32).astype(jnp.bfloat16)
    tile_of = lax.broadcasted_iota(jnp.int32, (T, R), 1) // TILE
    row_of = lax.broadcasted_iota(jnp.int32, (T, R), 0)
    part = []
    for span in spans:
        for tt in range(L):
            base = plan.block(s, c, span, tt) * (R // TILE)
            part.append(jnp.where(row_of == tile_of + base, 1.0, 0.0).astype(jnp.bfloat16))
    seen = jnp.dot(rows, jnp.concatenate(part, axis=1), preferred_element_type=jnp.float32)
    return jnp.where(seen > 0.5, 0.0, FLOOR)


def score_scale():
    return math.log2(math.e) / math.sqrt(HD)


def fill_keys(plan, spans, where, kv_refs, k_ref, v_ref):
    L, R = plan.L, plan.rows
    for m, span in enumerate(spans):
        for t in range(L):
            index, row = where[span, t]
            at = slice((m * L + t) * R, (m * L + t + 1) * R)
            k_ref[at, :] = kv_refs[index][row : row + R, :HD]
            v_ref[at, :HD] = kv_refs[index][row : row + R, HD:]
    v_ref[:, HD:] = jnp.ones((v_ref.shape[0], HD), jnp.bfloat16)


def attend_piece(plan, spans, t, s, c, mask, q_ref, k_ref, v_ref, s_ref, b_ref, write):
    L, G, R = plan.L, plan.group, plan.rows
    n, W, rts = len(spans), L * R, R // TILE
    scale = score_scale()
    b_ref[...] = tile_bias(plan, mask, s, c, spans, t)
    late = lax.broadcasted_iota(jnp.int32, (R, R), 1) > lax.broadcasted_iota(jnp.int32, (R, R), 0)
    corner = jnp.where(late, FLOOR, 0.0)
    for e in range(G):
        q = q_ref[:, (2 + e) * HD : (3 + e) * HD]
        high = None
        for m in range(n):
            sc = dot_nt(q, k_ref[m * W : (m + 1) * W, :])
            b = b_ref[:rts, m * W : (m + 1) * W]
            sc = (sc.reshape(rts, TILE, W) + b.reshape(rts, 1, W)).reshape(R, W)
            for tt in range(L):
                x = sc[:, tt * R : (tt + 1) * R]
                if spans[m] == (0, 0, 0) and tt == t:
                    x = x + corner
                s_ref[:, m * W + tt * R : m * W + (tt + 1) * R] = x
                high = x if high is None else jnp.maximum(high, x)
        top = jnp.max(high, axis=1, keepdims=True)
        total = None
        for m in range(n):
            w = jnp.exp2((s_ref[:, m * W : (m + 1) * W] - top) * scale).astype(jnp.bfloat16)
            d = jnp.dot(w, v_ref[m * W : (m + 1) * W, :], preferred_element_type=jnp.float32)
            total = d if total is None else total + d
        write(e, total, top)


def index_of(plan, spans, kv):
    arrays, where = [], {}
    for span in spans:
        for t in range(plan.L):
            array, row = kv[span, t]
            index = next((n for n, x in enumerate(arrays) if x is array), len(arrays))
            if index == len(arrays):
                arrays.append(array)
            where[span, t] = index, row
    return arrays, where


def stage_body(plan, spans, where, count, mask_ref, *refs):
    L, R = plan.L, plan.rows
    q_refs, refs = refs[:L], refs[L:]
    kv_refs, refs = refs[:count], refs[count:]
    out_refs, top_refs, (s_ref, b_ref, k_ref, v_ref) = refs[:L], refs[L : 2 * L], refs[2 * L :]
    s, c = lax.axis_index("seq"), lax.axis_index("head")
    fill_keys(plan, spans, where, kv_refs, k_ref, v_ref)
    for t in range(L):

        def write(e, total, top, t=t):
            out_refs[t][e * R : (e + 1) * R, :] = total
            top_refs[t][e * R : (e + 1) * R, :] = jnp.broadcast_to(top, (R, HD))

        attend_piece(plan, spans, t, s, c, mask_ref[...], q_refs[t], k_ref, v_ref, s_ref, b_ref, write)


def attend_stage(plan, spans, mask, q, kv):
    L, G, R = plan.L, plan.group, plan.rows
    arrays, where = index_of(plan, spans, kv)
    keys = len(spans) * L * R
    shapes = [jax.ShapeDtypeStruct((G * R, 2 * HD), jnp.float32)] * L
    shapes += [jax.ShapeDtypeStruct((G * R, HD), jnp.float32)] * L
    return pl.pallas_call(
        functools.partial(stage_body, plan, spans, where, len(arrays)),
        out_shape=shapes,
        in_specs=[VMEM] * (1 + L + len(arrays)),
        out_specs=[VMEM] * len(shapes),
        scratch_shapes=[
            pltpu.VMEM((R, keys), jnp.float32),
            pltpu.VMEM((8, keys), jnp.float32),
            pltpu.VMEM((keys, HD), jnp.bfloat16),
            pltpu.VMEM((keys, 2 * HD), jnp.bfloat16),
        ],
        compiler_params=pltpu.CompilerParams(vmem_limit_bytes=8 << 20),
        cost_estimate=pl.CostEstimate(flops=2 * L * G * R * keys * 3 * HD, bytes_accessed=0, transcendentals=0),
        name="stage",
    )(mask, *q, *arrays)


def far_body(plan, spans, t, where, count, mask_ref, q_ref, acc_ref, top_ref, *refs):
    R = plan.rows
    kv_refs, (out_ref, s_ref, b_ref, k_ref, v_ref) = refs[:count], refs[count:]
    s, c = lax.axis_index("seq"), lax.axis_index("head")
    a, _, _ = plan.split(s)
    scale = score_scale()

    def put(e, total):
        out_ref[:, e * HD : (e + 1) * HD] = (total[:, :HD] / total[:, HD:]).astype(jnp.bfloat16)

    def merge(e, total, top):
        at = slice(e * R, (e + 1) * R)
        old = top_ref[at, :1]
        high = jnp.maximum(old, top)
        put(e, acc_ref[at, :] * jnp.exp2((old - high) * scale) + total * jnp.exp2((top - high) * scale))

    @pl.when(a >= 1)
    def _():
        fill_keys(plan, spans, where, kv_refs, k_ref, v_ref)
        attend_piece(plan, spans, t, s, c, mask_ref[...], q_ref, k_ref, v_ref, s_ref, b_ref, merge)

    @pl.when(a < 1)
    def _():
        for e in range(plan.group):
            put(e, acc_ref[e * R : (e + 1) * R, :])


def attend_far(plan, spans, t, mask, q, kv, acc, top):
    L, G, R = plan.L, plan.group, plan.rows
    arrays, where = index_of(plan, spans, kv)
    keys = len(spans) * L * R
    return pl.pallas_call(
        functools.partial(far_body, plan, spans, t, where, len(arrays)),
        out_shape=jax.ShapeDtypeStruct((R, G * HD), jnp.bfloat16),
        in_specs=[VMEM] * (4 + len(arrays)),
        out_specs=VMEM,
        scratch_shapes=[
            pltpu.VMEM((R, keys), jnp.float32),
            pltpu.VMEM((8, keys), jnp.float32),
            pltpu.VMEM((keys, HD), jnp.bfloat16),
            pltpu.VMEM((keys, 2 * HD), jnp.bfloat16),
        ],
        compiler_params=pltpu.CompilerParams(vmem_limit_bytes=6 << 20),
        cost_estimate=pl.CostEstimate(flops=2 * G * R * keys * 3 * HD, bytes_accessed=0, transcendentals=0),
    )(mask, q, acc, top, *arrays)


def attend_staged(plan, spans, mask, q, kv):
    L, G, R = plan.L, plan.group, plan.rows
    step = max(1, STAGE // (L * R))
    parts = [attend_stage(plan, spans[n : n + step], mask, q, kv) for n in range(0, len(spans), step)]
    outs = []
    for t in range(L):
        top = functools.reduce(jnp.maximum, [p[L + t][:, :1] for p in parts])
        total = sum(p[t] * jnp.exp2((p[L + t][:, :1] - top) * score_scale()) for p in parts)
        o = (total[:, :HD] / total[:, HD:]).astype(jnp.bfloat16)
        outs.append(o.reshape(G, R, HD).transpose(1, 0, 2).reshape(R, G * HD))
    return outs


def hold_body(plan, t, w_ref, *refs):
    _, _, j = plan.split(lax.axis_index("seq"))
    if t == 0:
        mask_ref, out_ref, open_ref, raw_ref, sem = refs
    else:
        out_ref, sem = refs
    depth = out_ref.shape[0]
    here = pl.ds(pl.multiple_of((j + t) % plan.L * depth, depth), depth)
    copies = [pltpu.make_async_copy(w_ref.at[here, :], out_ref, sem.at[0])]
    if t == 0:
        copies.append(pltpu.make_async_copy(mask_ref, raw_ref, sem.at[1]))
    for copy in copies:
        copy.start()
    for copy in copies:
        copy.wait()
    if t == 0:
        open_ref[...] = raw_ref[...].astype(jnp.float32).astype(jnp.bfloat16)


def hold(plan, t, w, *mask):
    depth, D = w.shape[0] // plan.L, w.shape[1]
    size = w.size * w.dtype.itemsize
    shapes = [jax.ShapeDtypeStruct((depth, D), w.dtype)] + [jax.ShapeDtypeStruct(m.shape, jnp.bfloat16) for m in mask]
    return pl.pallas_call(
        functools.partial(hold_body, plan, t),
        out_shape=shapes,
        in_specs=[HBM] * (1 + len(mask)),
        out_specs=[VMEM] * len(shapes),
        scratch_shapes=[pltpu.VMEM(m.shape, m.dtype) for m in mask] + [pltpu.SemaphoreType.DMA((2,))],
        compiler_params=pltpu.CompilerParams(vmem_limit_bytes=GRANT - size * (6 + t) // 4),
        cost_estimate=pl.CostEstimate(flops=1 << 20, bytes_accessed=0, transcendentals=0),
    )(w, *mask)


def project_body(plan, cols, w_ref, a_ref, *refs):
    H, R = plan.H, plan.rows
    h = lax.axis_index("head")
    part = R // H
    for n in range(w_ref.shape[1] // cols):
        at = slice(n * cols, (n + 1) * cols)
        d = jnp.dot(a_ref[...], w_ref[:, at], preferred_element_type=jnp.float32)
        if len(refs) == 1:
            refs[0][:, at] = d
            continue
        sum_ref, send_ref, own_ref, all_ref = refs
        all_ref[:, at] = sum_ref[:, at] + d
        own_ref[:, at] = all_ref[pl.ds(pl.multiple_of(h * part, part), part), at]
        for u in range(1, H):
            to = (h + u) % H
            send_ref[(u - 1) * part : u * part, at] = all_ref[pl.ds(pl.multiple_of(to * part, part), part), at].astype(
                jnp.bfloat16
            )


def project(plan, t, piece, w, total):
    H, R = plan.H, plan.rows
    depth, D = piece.shape[1], w.shape[1]
    part = R // H
    last = t == plan.L - 1
    if last:
        shapes = [
            jax.ShapeDtypeStruct(((H - 1) * part, D), jnp.bfloat16),
            jax.ShapeDtypeStruct((part, D), jnp.float32),
        ]
    else:
        shapes = [jax.ShapeDtypeStruct((R, D), jnp.float32)]
    args = [w, piece] + ([total] if last else [])
    return pl.pallas_call(
        functools.partial(project_body, plan, 512),
        out_shape=shapes,
        in_specs=[VMEM] * len(args),
        out_specs=[VMEM] * len(shapes),
        scratch_shapes=[pltpu.VMEM((R, D), jnp.float32)] if last else [],
        compiler_params=pltpu.CompilerParams(vmem_limit_bytes=6 << 20),
        cost_estimate=pl.CostEstimate(flops=2 * R * depth * D, bytes_accessed=0, transcendentals=0),
        name="project",
    )(*args)


def layer(plan, queries, keys, values, tile_mask, out_weight):
    L, H, R = plan.L, plan.H, plan.rows
    wide = plan.group * HD
    _, _, j = plan.split(lax.axis_index("seq"))

    kv_send, full_send = [], []
    for t in range(L):
        p = (j + t) % L
        k_p = lax.dynamic_slice(keys, (0, p * HD), (R, HD))
        v_p = lax.dynamic_slice(values, (0, p * HD), (R, HD))
        q_p = lax.dynamic_slice(queries, (0, p * wide), (R, wide))
        kv_send.append(jnp.concatenate([k_p, v_p], axis=1))
        full_send.append(jnp.concatenate([k_p, v_p, q_p], axis=1))
    first_weight, mask = hold(plan, 0, out_weight, tile_mask)
    weights = [first_weight]
    for t in range(1, L):
        weights += hold(plan, t, out_weight)

    kv = {}
    side = plan.side_pairs()
    own = {}
    for k in [0, *plan.far()]:
        for t in range(L):
            own[k, t] = lax.ppermute(kv_send[t] if k else full_send[t], BOTH, plan.out_pairs(k, t))
    q = [own[0, t] for t in range(L)]
    near = jnp.concatenate([own[0, t][:, : 2 * HD] for t in range(L)], axis=0)
    near_side = lax.ppermute(near, BOTH, side)
    for t in range(L):
        kv[(0, 0, 0), t] = near, t * R
        kv[(0, 1, 0), t] = near_side, t * R
    both = jnp.concatenate([near, near_side], axis=0)
    for u in range(1, H):
        got = lax.ppermute(both, "head", plan.head_pairs(u))
        for t in range(L):
            kv[(0, 0, u), t] = got, t * R
            kv[(0, 1, u), t] = got, (L + t) * R
    for k in plan.far():
        far = jnp.concatenate([own[k, t] for t in range(L)], axis=0)
        far_side = lax.ppermute(far, BOTH, side)
        for n, block in enumerate((far, far_side)):
            got = {u: lax.ppermute(block, "head", plan.head_pairs(u)) for u in range(1, H)}
            for u in range(H):
                for t in range(L):
                    kv[(k, n, u), t] = got[u] if u else block, t * R
    spans = [(k, n, u) for k in [0, *plan.far()] for n in range(2) for u in range(H)]
    pieces = []
    if plan.A == 2:
        near_spans, far_spans = [x for x in spans if x[0] == 0], [x for x in spans if x[0]]
        state = attend_stage(plan, near_spans, mask, q, kv)
        for t in range(L):
            out = attend_far(plan, far_spans, t, mask, q[t], kv, state[t], state[L + t])
            pieces.append(lax.ppermute(out, BOTH, plan.back_pairs(t)))
    else:
        outs = attend_staged(plan, spans, mask, q, kv)
        for t in range(L):
            pieces.append(lax.ppermute(outs[t], BOTH, plan.back_pairs(t)))
    total = None
    for t in range(L):
        res = project(plan, t, pieces[t], weights[t], total)
        total = res[0]
    send, mine = res
    part = R // H
    for u in range(1, H):
        got = lax.ppermute(send[(u - 1) * part : u * part], "head", [(c, (c + u) % H) for c in range(H)])
        mine = mine + got.astype(jnp.float32)
    return mine.astype(jnp.bfloat16)


def solution(mesh):
    def program(queries, keys, values, tile_mask, out_weight):
        groups = keys.shape[1] // mesh.shape["head"] // HD
        rows = queries.shape[0] // mesh.shape["seq"]
        plan = Plan(mesh, groups, queries.shape[1] // keys.shape[1], rows, tile_mask.shape[0])

        def body(*args):
            return layer(plan, *args)

        step = jax.shard_map(
            body,
            mesh=mesh,
            in_specs=(P("seq", "head"), P("seq", "head"), P("seq", "head"), P(), P("head", None)),
            out_specs=P(("seq", "head"), None),
            check_vma=False,
        )
        return step(queries, keys, values, tile_mask, out_weight)

    return program
```
